32 devices in a mesh: elem: 16 (over z, y, core), band: 2 (over x).
Axes of the slice: x: 2, y: 2, z: 4, core: 2. Of those that a mesh axis runs over, the one named last changes fastest.
Arguments:
- y_current: bfloat16 [512, 64, 512], P('elem', None, 'band'), may hold values from -6 to 6
- y_previous: bfloat16 [512, 64, 512], P('elem', None, 'band'), may hold values from -6 to 6
- h_blocks: bfloat16 [512, 64, 320], P('elem'), may hold values from -0.3125 to 0.3125
- basis_sizes: int32 [512], P('elem'), may hold values from 40 to 64
- neighbours: int32 [512, 4], P('elem'), may hold values from 0 to 511, as said below
Outputs:
- filtered: bfloat16 [512, 64, 512], P('elem', None, 'band')
- margin: float32 [512, 512], P('elem', 'band')
The draws below stay inside these ranges and needn't reach their ends.
Inputs may be any that keep to these rules, and one draw needn't show every extreme that they name: `neighbours`: the elements lie on a periodic grid of 32 x 16; row i lists the elements that share an edge with element i, in the order previous grid row, next grid row, previous column, next column, so adjacency is symmetric. Element g belongs to index g // 32 of elem, whose elements fill 2 consecutive grid rows in some order; a neighbour therefore belongs to the same index or to one of the two beside it, periodically, and exactly 16 of an index's elements have a neighbour on the next index, and 16 on the previous one.
All inputs are finite; a program needn't handle non-finite values.
Results may differ from the reference program's by a relative error of at most 0.018.
Values may be sent and summed in bfloat16 or wider, within the bound.
A program may use at most 64 MiB of HBM per device.

```python
import jax
import jax.numpy as jnp
from jax import lax

BMAX = 64
SX = 2
GY = 16
BD = 256
DEGREES = 2
EL_DEV = 32
ELEMS = 512
NBAND = 512
N_ELEM = 16
N_BAND = 2


def draw_neighbours(key, part):
    keys = jax.random.split(jax.random.fold_in(key, 7), N_ELEM)

    def one_order(single):
        return jax.random.permutation(single, EL_DEV)
    orders = jax.vmap(one_order)(keys).astype(jnp.int32)
    owners = jnp.arange(N_ELEM, dtype=jnp.int32)[:, None] * EL_DEV
    grid = (owners + orders).reshape(SX * N_ELEM, GY)
    upper = jnp.roll(grid, 1, axis=0)
    lower = jnp.roll(grid, -1, axis=0)
    left_side = jnp.roll(grid, 1, axis=1)
    right_side = jnp.roll(grid, -1, axis=1)
    table = jnp.stack([upper, lower, left_side, right_side], axis=-1).reshape(-1, 4)
    return jnp.zeros((ELEMS, 4), jnp.int32).at[grid.reshape(-1)].set(table)


def with_ends(array, own_key, least, high):
    extent = array.shape
    place = [jax.random.randint(jax.random.fold_in(own_key, axis), (), 0, extent[axis]) for axis in range(len(extent))]
    array = array.at[tuple(place)].set(least)
    longest = extent.index(max(extent))
    place[longest] = (place[longest] + 1) % extent[longest]
    return array.at[tuple(place)].set(high)


def level_of(own_key, dims, cuts, smallest, top_value):
    def one(axis_at, parts):
        draws = jax.random.uniform(jax.random.fold_in(jax.random.fold_in(own_key, 6), axis_at), (parts,), jnp.float32, smallest / len(cuts), top_value / len(cuts))
        return jnp.repeat(jnp.exp(draws), dims[axis_at] // parts).reshape((-1,) + (1,) * (len(dims) - axis_at - 1))

    loudness = one(*cuts[0])
    for cut in cuts[1:]:
        loudness = loudness * one(*cut)
    return loudness


def bell_draw(key, dims, width, reach, cuts=(), held_as=jnp.bfloat16):
    drawn = width * jax.random.normal(key, dims, jnp.float32)
    if cuts:
        drawn = drawn * level_of(key, dims, cuts, -0.22, 0.18)
    return jnp.clip(drawn, -reach, reach).astype(held_as)


def setup_inputs(seed: int = 0) -> dict:
    key_list = jax.random.split(jax.random.key(seed), 6)
    y_current = bell_draw(key_list[0], (ELEMS, BMAX, NBAND), 1.0, 6.0, ((0, 16), (2, 2)))
    y_previous = bell_draw(key_list[1], (ELEMS, BMAX, NBAND), 1.0, 6.0, ((0, 16), (2, 2)))
    h_blocks = bell_draw(key_list[2], (ELEMS, BMAX, 5 * BMAX), (5 * BMAX) ** -0.5, 0.3125, ((0, 16),))
    basis_sizes = with_ends(jax.random.randint(key_list[3], (ELEMS,), BMAX * 5 // 8, BMAX + 1), jax.random.fold_in(key_list[3], 1), BMAX * 5 // 8, BMAX).astype(jnp.int32)
    neighbours = draw_neighbours(jax.random.fold_in(key_list[5], 71), 0)
    return dict(y_current=y_current, y_previous=y_previous, h_blocks=h_blocks, basis_sizes=basis_sizes, neighbours=neighbours)


center_value = 0.3
spectral_half = 1.7


def filter_block(pair, h_blocks, neighbours, row_mask):
    current, previous = pair
    current = current * row_mask
    previous = previous * row_mask
    hmatrix = h_blocks.astype(jnp.float32)
    mask_float = row_mask.astype(jnp.float32)
    for degree in range(DEGREES):
        nearby = current[neighbours]
        stacked = jnp.concatenate([current[:, None], nearby], axis=1)
        stacked = stacked.reshape(current.shape[0], 5 * BMAX, current.shape[2]).astype(jnp.float32)
        applied = jnp.einsum("irc,icb->irb", hmatrix, stacked, precision=lax.Precision.HIGHEST)
        following = mask_float * ((2.0 / spectral_half) * (applied - center_value * current.astype(jnp.float32)) - previous.astype(jnp.float32))
        previous = current
        current = following.astype(jnp.bfloat16)
    return current


def reference(y_current, y_previous, h_blocks, basis_sizes, neighbours):
    row_mask = (jnp.arange(BMAX, dtype=jnp.int32)[None, :] < basis_sizes[:, None]).astype(jnp.bfloat16)[:, :, None]

    def split_bands(values):
        return values.reshape(ELEMS, BMAX, N_BAND, BD).transpose(2, 0, 1, 3)

    def run_block(pair):
        return filter_block(pair, h_blocks, neighbours, row_mask)

    blocks = lax.map(run_block, (split_bands(y_current), split_bands(y_previous)))
    filtered = blocks.transpose(1, 2, 0, 3).reshape(ELEMS, BMAX, NBAND)
    flat = filtered.reshape(ELEMS * BMAX, NBAND).astype(jnp.float32)
    margin = jnp.dot(flat.T, flat, precision=lax.Precision.HIGHEST, preferred_element_type=jnp.float32)
    margin = margin / jnp.float32(ELEMS * BMAX)
    return filtered, margin
```

```python
import functools

import jax
import jax.numpy as jnp
from jax import lax
from jax.experimental import pallas as pl
from jax.experimental.pallas import tpu as pltpu
from jax.sharding import PartitionSpec as P

CHUNKS = 4
center_value = 0.3
spectral_half = 1.7
MESH = pl.DeviceIdType.MESH
ROWS = (((0,), (0,)), ((), ()))


def kernel(
    count_elem, count_band,
    pos_ref, perm_ref, neigh_ref, size_ref, cur_hbm, prev_hbm, h_hbm,
    out_hbm, margin_ref,
    cur, prev, h, y1, y2, f, ordered, halo, other, gram, cross,
    w, v, w1, v1, w2, v2, rw, rv,
    load_sem, out_sem, halo_send, halo_recv, x_send, x_recv,
    pair_send, pair_recv, w_send, w_recv, v_send, v_recv,
):
    e = lax.axis_index("elem")
    b = lax.axis_index("band")
    local, bmax, bands = y1.shape
    edge = local // 2
    q = edge // CHUNKS
    half = count_elem // 2
    rows = margin_ref.shape[0]
    per_block = bands // rows
    after = lax.rem(e + 1, count_elem)
    before = lax.rem(e + count_elem - 1, count_elem)
    parity = lax.rem(e, 2)
    pair = lax.div(e, 2)
    partner = e + 1 - 2 * parity

    loads = [
        pltpu.make_async_copy(src, dst, load_sem.at[k])
        for k, (src, dst) in enumerate(((cur_hbm, cur), (prev_hbm, prev), (h_hbm, h)))
    ]
    for load in loads:
        load.start()

    barrier = pltpu.get_barrier_semaphore()
    for target in (after, before):
        pl.semaphore_signal(barrier, inc=1, device_id=(target, b), device_id_type=MESH)
    for j in range(count_band):
        for d in range(half):
            if j or d:
                target = (2 * lax.rem(pair + d, half) + parity, lax.rem(b + j, count_band))
                pl.semaphore_signal(barrier, inc=1, device_id=target, device_id_type=MESH)

    row_index = lax.broadcasted_iota(jnp.int32, (bmax, bands), 0)

    loads[0].wait()

    def place(p, _):
        i = perm_ref[p]
        y1[p] = jnp.where(row_index < size_ref[i], cur[i].astype(jnp.float32), 0.0).astype(jnp.bfloat16)
        return 0

    lax.fori_loop(0, local, place, 0, unroll=4)
    pl.semaphore_wait(barrier, 2 + half * count_band - 1)

    def halo_copy(degree, side, c, source):
        return pltpu.make_async_remote_copy(
            src_ref=source.at[pl.ds(side * edge + c * q, q)],
            dst_ref=halo.at[degree, 1 - side, pl.ds(c * q, q)],
            send_sem=halo_send.at[degree, side, c],
            recv_sem=halo_recv.at[degree, 1 - side, c],
            device_id=(after if side else before, b),
            device_id_type=MESH,
        )

    def halo_arrived(degree, side, c):
        pltpu.make_async_remote_copy(
            src_ref=y1.at[pl.ds(0, q)],
            dst_ref=halo.at[degree, side, pl.ds(c * q, q)],
            send_sem=halo_send.at[degree, side, c],
            recv_sem=halo_recv.at[degree, side, c],
            device_id=(after if side else before, b),
            device_id_type=MESH,
        ).wait_recv()

    for c in range(CHUNKS):
        for side in (0, 1):
            halo_copy(0, side, c, y1).start()

    loads[1].wait()
    loads[2].wait()

    def element(degree, side, s, now, older, store):
        p = side * edge + s
        i = perm_ref[p]
        inner = now[pos_ref[lax.rem(neigh_ref[i, 1 - side], local)]]
        left = now[pos_ref[lax.rem(neigh_ref[i, 2], local)]]
        right = now[pos_ref[lax.rem(neigh_ref[i, 3], local)]]
        outer = halo[degree, side, s]
        mine = now[p]
        vertical = [inner, outer] if side else [outer, inner]
        stacked = jnp.concatenate([mine] + vertical + [left, right], axis=0)
        applied = jnp.dot(h[i], stacked, preferred_element_type=jnp.float32)
        following = (2.0 / spectral_half) * (
            applied - center_value * mine.astype(jnp.float32)
        ) - older(p, i).astype(jnp.float32)
        store[p] = jnp.where(row_index < size_ref[i], following, 0.0).astype(jnp.bfloat16)

    def first(c, _):
        halo_arrived(0, 0, c)
        halo_arrived(0, 1, c)
        for k in range(q):
            for side in (0, 1):
                element(0, side, c * q + k, y1, lambda p, i: prev[i], y2)
        for side in (0, 1):
            halo_copy(1, side, c, y2).start()
        return 0

    lax.fori_loop(0, CHUNKS, first, 0)

    gram[...] = jnp.zeros_like(gram)
    cross[...] = jnp.zeros_like(cross)

    def x_copy(j, c):
        to = lax.rem(b + j, count_band)
        start = jnp.where(to < b, 0, edge)
        return pltpu.make_async_remote_copy(
            src_ref=f.at[pl.ds(start + c * q, q)],
            dst_ref=other.at[count_band - j - 1, pl.ds(c * q, q)],
            send_sem=x_send.at[j - 1, c],
            recv_sem=x_recv.at[count_band - j - 1, c],
            device_id=(e, to),
            device_id_type=MESH,
        )

    def x_arrived(j, c):
        pltpu.make_async_remote_copy(
            src_ref=f.at[pl.ds(0, q)],
            dst_ref=other.at[j - 1, pl.ds(c * q, q)],
            send_sem=x_send.at[j - 1, c],
            recv_sem=x_recv.at[j - 1, c],
            device_id=(e, lax.rem(b + j, count_band)),
            device_id_type=MESH,
        ).wait_recv()

    def add_cross(c):
        for j in range(1, count_band):
            x_arrived(j, c)
            start = jnp.where(b < lax.rem(b + j, count_band), 0, edge)
            mine = f[pl.ds(start + c * q, q)].reshape(q * bmax, bands)
            theirs = other[j - 1, pl.ds(c * q, q)].reshape(q * bmax, bands)
            cross[j - 1] += lax.dot_general(mine, theirs, ROWS, preferred_element_type=jnp.float32)

    def second(c, _):
        halo_arrived(1, 0, c)
        halo_arrived(1, 1, c)
        for k in range(q):
            for side in (0, 1):
                element(1, side, c * q + k, y2, lambda p, i: y1[p], f)
        for j in range(1, count_band):
            x_copy(j, c).start()
        for side in (0, 1):
            block = f[pl.ds(side * edge + c * q, q)].reshape(q * bmax, bands)
            gram[...] += lax.dot_general(block, block, ROWS, preferred_element_type=jnp.float32)

        @pl.when(c > 0)
        def _():
            add_cross(c - 1)

        return 0

    lax.fori_loop(0, CHUNKS, second, 0)

    def give(i, _):
        ordered[i] = f[pos_ref[i]]
        return 0

    lax.fori_loop(0, local, give, 0, unroll=4)
    store = pltpu.make_async_copy(ordered, out_hbm, out_sem)
    store.start()

    def put_w(block, matrix):
        for k in range(per_block):
            w[k % 2, block * (per_block // 2) + k // 2] = matrix[k * rows:(k + 1) * rows].astype(jnp.bfloat16)

    put_w(b, gram[...])
    add_cross(CHUNKS - 1)
    for j in range(1, count_band):
        matrix = cross[j - 1]
        put_w(lax.rem(b + j, count_band), matrix.T)
        for k in range(per_block):
            v[k % 2, j - 1, k // 2] = matrix[k * rows:(k + 1) * rows].astype(jnp.bfloat16)

    def pair_copy(n, source, target):
        return pltpu.make_async_remote_copy(
            src_ref=source.at[1 - parity],
            dst_ref=target,
            send_sem=pair_send.at[n],
            recv_sem=pair_recv.at[n],
            device_id=(partner, b),
            device_id_type=MESH,
        )

    pairs = [pair_copy(0, w, w1), pair_copy(1, v, v1)]
    for copy in pairs:
        copy.start()
    pairs[0].wait_recv()
    w2[...] = (w[parity].astype(jnp.float32) + w1[...].astype(jnp.float32)).astype(jnp.bfloat16)
    pairs[1].wait_recv()
    v2[...] = (v[parity].astype(jnp.float32) + v1[...].astype(jnp.float32)).astype(jnp.bfloat16)

    def w_copy(d):
        to = lax.rem(pair + d, half)
        return pltpu.make_async_remote_copy(
            src_ref=w2.at[to],
            dst_ref=rw.at[half - d - 1],
            send_sem=w_send.at[d - 1],
            recv_sem=w_recv.at[half - d - 1],
            device_id=(2 * to + parity, b),
            device_id_type=MESH,
        )

    def v_copy(j, k):
        return pltpu.make_async_remote_copy(
            src_ref=v2.at[j - 1, k],
            dst_ref=rv.at[pair],
            send_sem=v_send.at[j - 1, k],
            recv_sem=v_recv.at[pair],
            device_id=(b * per_block + 2 * k + parity, lax.rem(b + j, count_band)),
            device_id_type=MESH,
        )

    sends = [w_copy(d) for d in range(1, half)]
    sends += [v_copy(j, k) for j in range(1, count_band) for k in range(per_block // 2)]
    for copy in sends:
        copy.start()

    margin_ref[...] = w2[pair].astype(jnp.float32)
    for d in range(1, half):
        pltpu.make_async_remote_copy(
            src_ref=w2.at[0],
            dst_ref=rw.at[d - 1],
            send_sem=w_send.at[d - 1],
            recv_sem=w_recv.at[d - 1],
            device_id=(2 * lax.rem(pair + d, half) + parity, b),
            device_id_type=MESH,
        ).wait_recv()
        margin_ref[...] += rw[d - 1].astype(jnp.float32)

    block = lax.div(e, per_block)

    @pl.when(block != b)
    def _():
        for k in range(half):
            pltpu.make_async_remote_copy(
                src_ref=v2.at[0, 0],
                dst_ref=rv.at[k],
                send_sem=v_send.at[0, 0],
                recv_sem=v_recv.at[k],
                device_id=(2 * k + parity, block),
                device_id_type=MESH,
            ).wait_recv()
            margin_ref[...] += rv[k].astype(jnp.float32)

    margin_ref[...] = margin_ref[...] / jnp.float32(local * count_elem * bmax)

    for copy in pairs + sends:
        copy.wait_send()

    def drain(c, _):
        for side in (0, 1):
            halo_copy(0, side, c, y1).wait_send()
            halo_copy(1, side, c, y2).wait_send()
        for j in range(1, count_band):
            x_copy(j, c).wait_send()
        return 0

    lax.fori_loop(0, CHUNKS, drain, 0)
    store.wait()


def edge_order(neighbours):
    local = neighbours.shape[0]
    owners = neighbours[:, 0] // local
    ids = jnp.arange(local, dtype=jnp.int32)
    above = neighbours[:, 0] % local
    key = jnp.where(owners != lax.axis_index("elem"), above, local + ids)
    pos = jnp.sum((key[None, :] < key[:, None]).astype(jnp.int32), axis=1)
    perm = jnp.sum(jnp.where(pos[None, :] == ids[:, None], ids[None, :], 0), axis=1)
    return pos, perm


def on_device(count_elem, count_band, y_current, y_previous, h_blocks, basis_sizes, neighbours):
    local, bmax, bands = y_current.shape
    rows = bands * count_band // count_elem
    per_block = bands // rows
    half = count_elem // 2
    pos, perm = edge_order(neighbours)
    smem = pl.BlockSpec(memory_space=pltpu.SMEM)
    anywhere = pl.BlockSpec(memory_space=pl.ANY)
    bf16, f32 = jnp.bfloat16, jnp.float32
    dma = pltpu.SemaphoreType.DMA
    whole = (local, bmax, bands)
    others = count_band - 1
    slot = (rows, bands)
    return tuple(pl.pallas_call(
        functools.partial(kernel, count_elem, count_band),
        out_shape=(
            jax.ShapeDtypeStruct(whole, bf16),
            jax.ShapeDtypeStruct((rows, bands), f32),
        ),
        in_specs=[smem] * 4 + [anywhere] * 3,
        out_specs=(anywhere, pl.BlockSpec(memory_space=pltpu.VMEM)),
        scratch_shapes=[
            pltpu.VMEM(whole, bf16),
            pltpu.VMEM(whole, bf16),
            pltpu.VMEM(h_blocks.shape, bf16),
            pltpu.VMEM(whole, bf16),
            pltpu.VMEM(whole, bf16),
            pltpu.VMEM(whole, bf16),
            pltpu.VMEM(whole, bf16),
            pltpu.VMEM((2, 2, local // 2, bmax, bands), bf16),
            pltpu.VMEM((others, local // 2, bmax, bands), bf16),
            pltpu.VMEM((bands, bands), f32),
            pltpu.VMEM((others, bands, bands), f32),
            pltpu.VMEM((2, half) + slot, bf16),
            pltpu.VMEM((2, others, per_block // 2) + slot, bf16),
            pltpu.VMEM((half,) + slot, bf16),
            pltpu.VMEM((others, per_block // 2) + slot, bf16),
            pltpu.VMEM((half,) + slot, bf16),
            pltpu.VMEM((others, per_block // 2) + slot, bf16),
            pltpu.VMEM((half - 1,) + slot, bf16),
            pltpu.VMEM((half,) + slot, bf16),
            dma((3,)),
            dma,
            dma((2, 2, CHUNKS)),
            dma((2, 2, CHUNKS)),
            dma((others, CHUNKS)),
            dma((others, CHUNKS)),
            dma((2,)),
            dma((2,)),
            dma((half - 1,)),
            dma((half - 1,)),
            dma((others, per_block // 2)),
            dma((half,)),
        ],
        compiler_params=pltpu.CompilerParams(
            collective_id=0, has_side_effects=True, vmem_limit_bytes=48 * 1024 * 1024
        ),
    )(pos, perm, neighbours, basis_sizes, y_current, y_previous, h_blocks))


def solution(mesh):
    in_specs = (
        P("elem", None, "band"),
        P("elem", None, "band"),
        P("elem", None, None),
        P("elem"),
        P("elem", None),
    )
    out_specs = (P("elem", None, "band"), P("elem", "band"))
    body = functools.partial(on_device, mesh.shape["elem"], mesh.shape["band"])
    return jax.shard_map(body, mesh=mesh, in_specs=in_specs, out_specs=out_specs, check_vma=False)
```

```python
import functools

import jax
import jax.numpy as jnp
from jax import lax
from jax.experimental import pallas as pl
from jax.experimental.pallas import tpu as pltpu
from jax.sharding import PartitionSpec as P

GROUP = 2
center_value = 0.3
spectral_half = 1.7
MESH = pl.DeviceIdType.MESH
ROWS = (((0,), (0,)), ((), ()))


def kernel(
    count_elem, count_band,
    neigh_hbm, size_hbm, cur_hbm, prev_hbm, h_hbm,
    out_hbm, margin_ref,
    neigh_vec, table_vec, neigh_ref, size_ref, table,
    cur, prev, h, y1, y2, f, ordered, halo, other, gram, cross,
    w, v, w1, v1, w2, v2, rw, rv,
    load_sem, out_sem, halo_send, halo_recv, x_send, x_recv,
    pair_send, pair_recv, w_send, w_recv, v_send, v_recv,
):
    e = lax.axis_index("elem")
    b = lax.axis_index("band")
    local, bmax, bands = y1.shape
    edge = local // 2
    q = GROUP
    chunks = edge // q
    half = count_elem // 2
    rows = margin_ref.shape[0]
    per_block = bands // rows
    parity = lax.rem(e, 2)
    pair = lax.div(e, 2)
    fast, slow = 1 - parity, parity
    partner = e + 1 - 2 * parity
    neighbour = lax.rem(e + count_elem - 1 + 2 * parity, count_elem)

    sources = (neigh_hbm, neigh_hbm, size_hbm, cur_hbm, prev_hbm, h_hbm)
    targets = (neigh_vec, neigh_ref, size_ref, cur, prev, h)
    loads = [
        pltpu.make_async_copy(source, target, load_sem.at[k])
        for k, (source, target) in enumerate(zip(sources, targets))
    ]
    for load in loads:
        load.start()

    barrier = pltpu.get_barrier_semaphore()
    for target in (neighbour, partner):
        pl.semaphore_signal(barrier, inc=1, device_id=(target, b), device_id_type=MESH)
    for j in range(count_band):
        for d in range(half):
            if j or d:
                target = (2 * lax.rem(pair + d, half) + parity, lax.rem(b + j, count_band))
                pl.semaphore_signal(barrier, inc=1, device_id=target, device_id_type=MESH)

    loads[0].wait()
    above = neigh_vec[0:1, :]
    lane = lax.broadcasted_iota(jnp.int32, (1, local), 1)
    key = jnp.where(lax.div(above, local) != e, lax.rem(above, local), local + lane)
    key = key * local + lane
    key_row = jnp.broadcast_to(key, (local, local))
    down = lax.broadcasted_iota(jnp.int32, (local, local), 0)
    across = lax.broadcasted_iota(jnp.int32, (local, local), 1)
    key_col = jnp.sum(jnp.where(down == across, key_row, 0), axis=1, keepdims=True)
    pos_row = jnp.sum(jnp.where(key_col < key_row, 1, 0), axis=0, keepdims=True)
    pos_col = jnp.sum(jnp.where(key_row < key_col, 1, 0), axis=1, keepdims=True)
    perm_row = jnp.sum(jnp.where(pos_col == across, down, 0), axis=0, keepdims=True)
    table_vec[0:1, 0:local] = pos_row
    table_vec[1:2, 0:local] = perm_row
    order = pltpu.make_async_copy(table_vec, table, load_sem.at[len(loads)])
    order.start()

    row_index = lax.broadcasted_iota(jnp.int32, (bmax, bands), 0)

    for load in loads[1:4]:
        load.wait()
    order.wait()

    def place(start):
        def one(k, _):
            p = start + k
            i = table[1, p]
            y1[p] = jnp.where(row_index < size_ref[i], cur[i].astype(jnp.float32), 0.0).astype(jnp.bfloat16)
            return 0

        lax.fori_loop(0, edge, one, 0, unroll=4)

    def slow_copy(degree, c, source):
        return pltpu.make_async_remote_copy(
            src_ref=source.at[pl.ds(slow * edge + c * q, q)],
            dst_ref=halo.at[degree, 0, pl.ds(c * q, q)],
            send_sem=halo_send.at[degree, c],
            recv_sem=halo_recv.at[degree, c],
            device_id=(neighbour, b),
            device_id_type=MESH,
        )

    def fast_copy(degree, source):
        return pltpu.make_async_remote_copy(
            src_ref=source.at[pl.ds(fast * edge, edge)],
            dst_ref=halo.at[degree, 1],
            send_sem=halo_send.at[degree, chunks],
            recv_sem=halo_recv.at[degree, chunks],
            device_id=(partner, b),
            device_id_type=MESH,
        )

    place(slow * edge)
    pl.semaphore_wait(barrier, 2 + half * count_band - 1)
    for c in range(chunks):
        slow_copy(0, c, y1).start()
    place(fast * edge)
    fast_copy(0, y1).start()

    loads[4].wait()
    loads[5].wait()

    def element(degree, side, s, now, older, store):
        p = side * edge + s
        i = table[1, p]
        inner = now[table[0, lax.rem(neigh_ref[1 - side, i], local)]]
        left = now[table[0, lax.rem(neigh_ref[2, i], local)]]
        right = now[table[0, lax.rem(neigh_ref[3, i], local)]]
        outer = halo[degree, jnp.where(side == fast, 1, 0), s]
        mine = now[p]
        upper = jnp.where(side == 0, outer, inner)
        lower = jnp.where(side == 0, inner, outer)
        stacked = jnp.concatenate([mine, upper, lower, left, right], axis=0)
        applied = jnp.dot(h[i], stacked, preferred_element_type=jnp.float32)
        following = (2.0 / spectral_half) * (
            applied - center_value * mine.astype(jnp.float32)
        ) - older(p, i).astype(jnp.float32)
        store[p] = jnp.where(row_index < size_ref[i], following, 0.0).astype(jnp.bfloat16)

    def older_first(p, i):
        return prev[i]

    def older_second(p, i):
        return y1[p]

    def first_fast(g, _):
        for k in range(4):
            element(0, fast, g * 4 + k, y1, older_first, y2)
        return 0

    fast_copy(0, y1).wait_recv()
    lax.fori_loop(0, edge // 4, first_fast, 0)
    fast_copy(1, y2).start()

    def first_slow(c, _):
        slow_copy(0, c, y1).wait_recv()
        for k in range(q):
            element(0, slow, c * q + k, y1, older_first, y2)
        slow_copy(1, c, y2).start()
        return 0

    lax.fori_loop(0, chunks, first_slow, 0)

    gram[...] = jnp.zeros_like(gram)
    cross[...] = jnp.zeros_like(cross)

    def sent_side(j):
        return jnp.where(lax.rem(b + j, count_band) < b, 0, 1)

    def x_copy(j, c):
        return pltpu.make_async_remote_copy(
            src_ref=f.at[pl.ds(sent_side(j) * edge + c * q, q)],
            dst_ref=other.at[count_band - j - 1, pl.ds(c * q, q)],
            send_sem=x_send.at[j - 1, c],
            recv_sem=x_recv.at[count_band - j - 1, c],
            device_id=(e, lax.rem(b + j, count_band)),
            device_id_type=MESH,
        )

    def x_start(side, c):
        for j in range(1, count_band):
            @pl.when(sent_side(j) == side)
            def _():
                x_copy(j, c).start()

    def x_arrived(j, c):
        pltpu.make_async_remote_copy(
            src_ref=f.at[pl.ds(0, q)],
            dst_ref=other.at[j - 1, pl.ds(c * q, q)],
            send_sem=x_send.at[j - 1, c],
            recv_sem=x_recv.at[j - 1, c],
            device_id=(e, lax.rem(b + j, count_band)),
            device_id_type=MESH,
        ).wait_recv()

    def add_gram(first, count):
        block = f[pl.ds(first, count)].reshape(count * bmax, bands)
        gram[...] += lax.dot_general(block, block, ROWS, preferred_element_type=jnp.float32)

    def add_cross(c):
        for j in range(1, count_band):
            x_arrived(j, c)
            start = (1 - sent_side(j)) * edge
            mine = f[pl.ds(start + c * q, q)].reshape(q * bmax, bands)
            theirs = other[j - 1, pl.ds(c * q, q)].reshape(q * bmax, bands)
            cross[j - 1] += lax.dot_general(mine, theirs, ROWS, preferred_element_type=jnp.float32)

    fast_copy(1, y2).wait_recv()

    def second_fast(g, _):
        for k in range(4):
            element(1, fast, g * 4 + k, y2, older_second, f)
        for k in range(4 // q):
            x_start(fast, g * (4 // q) + k)
        return 0

    lax.fori_loop(0, edge // 4, second_fast, 0)

    def gram_fast(g, _):
        add_gram(fast * edge + g * 4, 4)
        return 0

    lax.fori_loop(0, edge // 4, gram_fast, 0)

    def second_slow(c, _):
        slow_copy(1, c, y2).wait_recv()
        for k in range(q):
            element(1, slow, c * q + k, y2, older_second, f)
        x_start(slow, c)
        add_gram(slow * edge + c * q, q)

        @pl.when(c > 0)
        def _():
            add_cross(c - 1)

        return 0

    lax.fori_loop(0, chunks, second_slow, 0)

    def give(i, _):
        ordered[i] = f[table[0, i]]
        return 0

    lax.fori_loop(0, local, give, 0, unroll=4)
    store = pltpu.make_async_copy(ordered, out_hbm, out_sem)
    store.start()

    def put_w(block, matrix):
        for k in range(per_block):
            w[k % 2, block * (per_block // 2) + k // 2] = matrix[k * rows:(k + 1) * rows].astype(jnp.bfloat16)

    put_w(b, gram[...])
    add_cross(chunks - 1)
    for j in range(1, count_band):
        matrix = cross[j - 1]
        put_w(lax.rem(b + j, count_band), matrix.T)
        for k in range(per_block):
            v[k % 2, j - 1, k // 2] = matrix[k * rows:(k + 1) * rows].astype(jnp.bfloat16)

    def pair_copy(n, source, target):
        return pltpu.make_async_remote_copy(
            src_ref=source.at[1 - parity],
            dst_ref=target,
            send_sem=pair_send.at[n],
            recv_sem=pair_recv.at[n],
            device_id=(partner, b),
            device_id_type=MESH,
        )

    pairs = [pair_copy(0, w, w1), pair_copy(1, v, v1)]
    for copy in pairs:
        copy.start()
    pairs[0].wait_recv()
    w2[...] = (w[parity].astype(jnp.float32) + w1[...].astype(jnp.float32)).astype(jnp.bfloat16)
    pairs[1].wait_recv()
    v2[...] = (v[parity].astype(jnp.float32) + v1[...].astype(jnp.float32)).astype(jnp.bfloat16)

    def w_copy(d):
        to = lax.rem(pair + d, half)
        return pltpu.make_async_remote_copy(
            src_ref=w2.at[to],
            dst_ref=rw.at[half - d - 1],
            send_sem=w_send.at[d - 1],
            recv_sem=w_recv.at[half - d - 1],
            device_id=(2 * to + parity, b),
            device_id_type=MESH,
        )

    def v_copy(j, k):
        return pltpu.make_async_remote_copy(
            src_ref=v2.at[j - 1, k],
            dst_ref=rv.at[pair],
            send_sem=v_send.at[j - 1, k],
            recv_sem=v_recv.at[pair],
            device_id=(b * per_block + 2 * k + parity, lax.rem(b + j, count_band)),
            device_id_type=MESH,
        )

    sends = [w_copy(d) for d in range(1, half)]
    sends += [v_copy(j, k) for j in range(1, count_band) for k in range(per_block // 2)]
    for copy in sends:
        copy.start()

    margin_ref[...] = w2[pair].astype(jnp.float32)
    for d in range(1, half):
        pltpu.make_async_remote_copy(
            src_ref=w2.at[0],
            dst_ref=rw.at[d - 1],
            send_sem=w_send.at[d - 1],
            recv_sem=w_recv.at[d - 1],
            device_id=(2 * lax.rem(pair + d, half) + parity, b),
            device_id_type=MESH,
        ).wait_recv()
        margin_ref[...] += rw[d - 1].astype(jnp.float32)

    block = lax.div(e, per_block)

    @pl.when(block != b)
    def _():
        for k in range(half):
            pltpu.make_async_remote_copy(
                src_ref=v2.at[0, 0],
                dst_ref=rv.at[k],
                send_sem=v_send.at[0, 0],
                recv_sem=v_recv.at[k],
                device_id=(2 * k + parity, block),
                device_id_type=MESH,
            ).wait_recv()
            margin_ref[...] += rv[k].astype(jnp.float32)

    margin_ref[...] = margin_ref[...] / jnp.float32(local * count_elem * bmax)

    for copy in pairs + sends:
        copy.wait_send()

    fast_copy(0, y1).wait_send()
    fast_copy(1, y2).wait_send()

    def drain(c, _):
        slow_copy(0, c, y1).wait_send()
        slow_copy(1, c, y2).wait_send()
        for j in range(1, count_band):
            x_copy(j, c).wait_send()
        return 0

    lax.fori_loop(0, chunks, drain, 0)
    store.wait()


def on_device(count_elem, count_band, y_current, y_previous, h_blocks, basis_sizes, neighbours):
    local, bmax, bands = y_current.shape
    rows = bands * count_band // count_elem
    per_block = bands // rows
    half = count_elem // 2
    smem = pltpu.SMEM
    chunks = local // 2 // GROUP
    fixed = pl.BlockSpec(memory_space=pltpu.HBM)
    anywhere = pl.BlockSpec(memory_space=pl.ANY)
    bf16, f32 = jnp.bfloat16, jnp.float32
    dma = pltpu.SemaphoreType.DMA
    whole = (local, bmax, bands)
    others = count_band - 1
    slot = (rows, bands)
    return tuple(pl.pallas_call(
        functools.partial(kernel, count_elem, count_band),
        out_shape=(
            jax.ShapeDtypeStruct(whole, bf16),
            jax.ShapeDtypeStruct((rows, bands), f32),
        ),
        in_specs=[fixed] * 5,
        out_specs=(anywhere, pl.BlockSpec(memory_space=pltpu.VMEM)),
        scratch_shapes=[
            pltpu.VMEM((4, local), jnp.int32),
            pltpu.VMEM((8, 128), jnp.int32),
            smem((4, local), jnp.int32),
            smem((local,), jnp.int32),
            smem((8, 128), jnp.int32),
            pltpu.VMEM(whole, bf16),
            pltpu.VMEM(whole, bf16),
            pltpu.VMEM(h_blocks.shape, bf16),
            pltpu.VMEM(whole, bf16),
            pltpu.VMEM(whole, bf16),
            pltpu.VMEM(whole, bf16),
            pltpu.VMEM(whole, bf16),
            pltpu.VMEM((2, 2, local // 2, bmax, bands), bf16),
            pltpu.VMEM((others, local // 2, bmax, bands), bf16),
            pltpu.VMEM((bands, bands), f32),
            pltpu.VMEM((others, bands, bands), f32),
            pltpu.VMEM((2, half) + slot, bf16),
            pltpu.VMEM((2, others, per_block // 2) + slot, bf16),
            pltpu.VMEM((half,) + slot, bf16),
            pltpu.VMEM((others, per_block // 2) + slot, bf16),
            pltpu.VMEM((half,) + slot, bf16),
            pltpu.VMEM((others, per_block // 2) + slot, bf16),
            pltpu.VMEM((half - 1,) + slot, bf16),
            pltpu.VMEM((half,) + slot, bf16),
            dma((7,)),
            dma,
            dma((2, chunks + 1)),
            dma((2, chunks + 1)),
            dma((others, chunks)),
            dma((others, chunks)),
            dma((2,)),
            dma((2,)),
            dma((half - 1,)),
            dma((half - 1,)),
            dma((others, per_block // 2)),
            dma((half,)),
        ],
        compiler_params=pltpu.CompilerParams(
            collective_id=0, has_side_effects=True, vmem_limit_bytes=67_000_000
        ),
    )(neighbours.T, basis_sizes, y_current, y_previous, h_blocks))


def solution(mesh):
    in_specs = (
        P("elem", None, "band"),
        P("elem", None, "band"),
        P("elem", None, None),
        P("elem"),
        P("elem", None),
    )
    out_specs = (P("elem", None, "band"), P("elem", "band"))
    body = functools.partial(on_device, mesh.shape["elem"], mesh.shape["band"])
    return jax.shard_map(body, mesh=mesh, in_specs=in_specs, out_specs=out_specs, check_vma=False)
```

```python
import functools

import jax
import jax.numpy as jnp
from jax import lax
from jax.experimental import pallas as pl
from jax.experimental.pallas import tpu as pltpu
from jax.sharding import PartitionSpec as P

GROUP = 2
center_value = 0.3
spectral_half = 1.7
MESH = pl.DeviceIdType.MESH
ROWS = (((0,), (0,)), ((), ()))


def kernel(
    count_elem, count_band,
    neigh_hbm, size_hbm, cur_hbm, prev_hbm, h_hbm,
    out_ref, margin_ref,
    neigh_vec, table_vec, neigh_ref, size_ref, table,
    cur, prev, h, y1, y2, f, halo, other, gram, cross,
    w, w1, w2, rw, rv,
    load_sem, halo_send, halo_recv, x_send, x_recv,
    pair_send, pair_recv, w_send, w_recv, v_send, v_recv, far,
):
    e = lax.axis_index("elem")
    b = lax.axis_index("band")
    local, bmax, bands = y1.shape
    edge = local // 2
    q = GROUP
    chunks = edge // q
    half = count_elem // 2
    rows = margin_ref.shape[0]
    per_block = bands // rows
    parity = lax.rem(e, 2)
    pair = lax.div(e, 2)
    fast, slow = 1 - parity, parity
    partner = e + 1 - 2 * parity
    neighbour = lax.rem(e + count_elem - 1 + 2 * parity, count_elem)

    sources = (neigh_hbm, neigh_hbm, size_hbm, cur_hbm, prev_hbm, h_hbm)
    targets = (neigh_vec, neigh_ref, size_ref, cur, prev, h)
    loads = [
        pltpu.make_async_copy(source, target, load_sem.at[k])
        for k, (source, target) in enumerate(zip(sources, targets))
    ]
    for load in loads:
        load.start()

    barrier = pltpu.get_barrier_semaphore()
    for target in (neighbour, partner):
        pl.semaphore_signal(barrier, inc=1, device_id=(target, b), device_id_type=MESH)
    for j in range(1, count_band):
        pl.semaphore_signal(
            barrier, inc=1, device_id=(e, lax.rem(b + j, count_band)), device_id_type=MESH
        )

    reach = [1]
    while 2 * reach[-1] < half:
        reach.append(2 * reach[-1])

    def advance(step):
        if 0 < step <= len(reach):
            pl.semaphore_wait(far.at[step - 1], 2)
        elif step == len(reach) + 1:
            pl.semaphore_wait(far.at[step - 1], count_band - 1)
        if step < len(reach):
            for distance in (reach[step], count_elem - reach[step]):
                target = (lax.rem(e + distance, count_elem), b)
                pl.semaphore_signal(far.at[step], inc=1, device_id=target, device_id_type=MESH)
        elif step == len(reach):
            for j in range(1, count_band):
                target = (e, lax.rem(b + j, count_band))
                pl.semaphore_signal(far.at[step], inc=1, device_id=target, device_id_type=MESH)

    loads[0].wait()
    above = neigh_vec[0:1, :]
    lane = lax.broadcasted_iota(jnp.int32, (1, local), 1)
    key = jnp.where(lax.div(above, local) != e, lax.rem(above, local), local + lane)
    key = key * local + lane
    key_row = jnp.broadcast_to(key, (local, local))
    down = lax.broadcasted_iota(jnp.int32, (local, local), 0)
    across = lax.broadcasted_iota(jnp.int32, (local, local), 1)
    key_col = jnp.sum(jnp.where(down == across, key_row, 0), axis=1, keepdims=True)
    pos_row = jnp.sum(jnp.where(key_col < key_row, 1, 0), axis=0, keepdims=True)
    pos_col = jnp.sum(jnp.where(key_row < key_col, 1, 0), axis=1, keepdims=True)
    perm_row = jnp.sum(jnp.where(pos_col == across, down, 0), axis=0, keepdims=True)
    table_vec[0:1, 0:local] = pos_row
    table_vec[1:2, 0:local] = perm_row
    order = pltpu.make_async_copy(table_vec, table, load_sem.at[len(loads)])
    order.start()

    row_index = lax.broadcasted_iota(jnp.int32, (bmax, bands), 0)

    for load in loads[1:4]:
        load.wait()
    order.wait()

    def place(start):
        def one(k, _):
            p = start + k
            i = table[1, p]
            y1[p] = jnp.where(row_index < size_ref[i], cur[i].astype(jnp.float32), 0.0).astype(jnp.bfloat16)
            return 0

        lax.fori_loop(0, edge, one, 0, unroll=4)

    def slow_copy(degree, c, source):
        return pltpu.make_async_remote_copy(
            src_ref=source.at[pl.ds(slow * edge + c * q, q)],
            dst_ref=halo.at[degree, 0, pl.ds(c * q, q)],
            send_sem=halo_send.at[degree, c],
            recv_sem=halo_recv.at[degree, c],
            device_id=(neighbour, b),
            device_id_type=MESH,
        )

    def fast_copy(degree, source):
        return pltpu.make_async_remote_copy(
            src_ref=source.at[pl.ds(fast * edge, edge)],
            dst_ref=halo.at[degree, 1],
            send_sem=halo_send.at[degree, chunks],
            recv_sem=halo_recv.at[degree, chunks],
            device_id=(partner, b),
            device_id_type=MESH,
        )

    place(slow * edge)
    pl.semaphore_wait(barrier, 1 + count_band)
    for c in range(chunks):
        slow_copy(0, c, y1).start()
    place(fast * edge)
    fast_copy(0, y1).start()
    advance(0)

    loads[4].wait()
    loads[5].wait()

    def element(degree, side, s, now, older, store):
        p = side * edge + s
        i = table[1, p]
        inner = now[table[0, lax.rem(neigh_ref[1 - side, i], local)]]
        left = now[table[0, lax.rem(neigh_ref[2, i], local)]]
        right = now[table[0, lax.rem(neigh_ref[3, i], local)]]
        outer = halo[degree, jnp.where(side == fast, 1, 0), s]
        mine = now[p]
        upper = jnp.where(side == 0, outer, inner)
        lower = jnp.where(side == 0, inner, outer)
        stacked = jnp.concatenate([mine, upper, lower, left, right], axis=0)
        applied = jnp.dot(h[i], stacked, preferred_element_type=jnp.float32)
        following = (2.0 / spectral_half) * (
            applied - center_value * mine.astype(jnp.float32)
        ) - older(p, i).astype(jnp.float32)
        store[p] = jnp.where(row_index < size_ref[i], following, 0.0).astype(jnp.bfloat16)

    def older_first(p, i):
        return prev[i]

    def older_second(p, i):
        return y1[p]

    def first_fast(g, _):
        for k in range(4):
            element(0, fast, g * 4 + k, y1, older_first, y2)
        return 0

    fast_copy(0, y1).wait_recv()
    lax.fori_loop(0, edge // 4, first_fast, 0)
    fast_copy(1, y2).start()
    advance(1)

    def first_slow(c, _):
        slow_copy(0, c, y1).wait_recv()
        for k in range(q):
            element(0, slow, c * q + k, y1, older_first, y2)
        slow_copy(1, c, y2).start()
        return 0

    lax.fori_loop(0, chunks, first_slow, 0)
    advance(2)

    gram[...] = jnp.zeros_like(gram)
    cross[...] = jnp.zeros_like(cross)

    def sent_side(j):
        return jnp.where(lax.rem(b + j, count_band) < b, 0, 1)

    def x_copy(j, c):
        return pltpu.make_async_remote_copy(
            src_ref=f.at[pl.ds(sent_side(j) * edge + c * q, q)],
            dst_ref=other.at[count_band - j - 1, pl.ds(c * q, q)],
            send_sem=x_send.at[j - 1, c],
            recv_sem=x_recv.at[count_band - j - 1, c],
            device_id=(e, lax.rem(b + j, count_band)),
            device_id_type=MESH,
        )

    def x_start(side, c):
        for j in range(1, count_band):
            @pl.when(sent_side(j) == side)
            def _():
                x_copy(j, c).start()

    def x_arrived(j, c):
        pltpu.make_async_remote_copy(
            src_ref=f.at[pl.ds(0, q)],
            dst_ref=other.at[j - 1, pl.ds(c * q, q)],
            send_sem=x_send.at[j - 1, c],
            recv_sem=x_recv.at[j - 1, c],
            device_id=(e, lax.rem(b + j, count_band)),
            device_id_type=MESH,
        ).wait_recv()

    def add_gram(first, count):
        block = f[pl.ds(first, count)].reshape(count * bmax, bands)
        gram[...] += lax.dot_general(block, block, ROWS, preferred_element_type=jnp.float32)

    def add_cross(c):
        for j in range(1, count_band):
            x_arrived(j, c)
            start = (1 - sent_side(j)) * edge
            mine = f[pl.ds(start + c * q, q)].reshape(q * bmax, bands)
            theirs = other[j - 1, pl.ds(c * q, q)].reshape(q * bmax, bands)
            cross[j - 1] += lax.dot_general(mine, theirs, ROWS, preferred_element_type=jnp.float32)

    fast_copy(1, y2).wait_recv()

    def second_fast(g, _):
        for k in range(4):
            element(1, fast, g * 4 + k, y2, older_second, f)
        for k in range(4 // q):
            x_start(fast, g * (4 // q) + k)
        return 0

    lax.fori_loop(0, edge // 4, second_fast, 0)
    advance(3)

    def gram_fast(g, _):
        add_gram(fast * edge + g * 4, 4)
        return 0

    lax.fori_loop(0, edge // 4, gram_fast, 0)

    def second_slow(c, _):
        slow_copy(1, c, y2).wait_recv()
        for k in range(q):
            element(1, slow, c * q + k, y2, older_second, f)
        x_start(slow, c)
        add_gram(slow * edge + c * q, q)

        @pl.when(c > 0)
        def _():
            add_cross(c - 1)

        return 0

    lax.fori_loop(0, chunks, second_slow, 0)

    def cut(target, matrix):
        for k in range(per_block):
            w[k % 2, target, k // 2] = matrix[k * rows:(k + 1) * rows].astype(jnp.bfloat16)

    def pair_copy(n, first, count):
        return pltpu.make_async_remote_copy(
            src_ref=w.at[1 - parity, pl.ds(first, count)],
            dst_ref=w1.at[pl.ds(first, count)],
            send_sem=pair_send.at[n],
            recv_sem=pair_recv.at[n],
            device_id=(partner, b),
            device_id_type=MESH,
        )

    def pair_sum(n):
        w2[n] = (w[parity, n].astype(jnp.float32) + w1[n].astype(jnp.float32)).astype(jnp.bfloat16)

    others = count_band - 1

    def w_copy(j, k):
        to = lax.rem(b + j, count_band) * (per_block // 2) + k
        return to, pltpu.make_async_remote_copy(
            src_ref=w2.at[j, k],
            dst_ref=rw.at[pair],
            send_sem=w_send.at[j, k],
            recv_sem=w_recv.at[pair],
            device_id=(2 * to + parity, b),
            device_id_type=MESH,
        )

    def v_copy(j, k):
        return pltpu.make_async_remote_copy(
            src_ref=w2.at[others + j, k],
            dst_ref=rv.at[pair],
            send_sem=v_send.at[j - 1, k],
            recv_sem=v_recv.at[pair],
            device_id=(b * per_block + 2 * k + parity, lax.rem(b + j, count_band)),
            device_id_type=MESH,
        )

    def each_w(blocks, act):
        for j in blocks:
            for k in range(per_block // 2):
                to, copy = w_copy(j, k)

                @pl.when(to != pair)
                def _():
                    act(copy)

    def start(copy):
        copy.start()

    def sent(copy):
        copy.wait_send()

    cut(0, gram[...])
    pairs = [pair_copy(0, 0, 1), pair_copy(1, 1, 2 * others)]
    pairs[0].start()

    for step in range(4, len(reach) + 2):
        advance(step)

    def give(i, _):
        out_ref[i] = f[table[0, i]]
        return 0

    lax.fori_loop(0, local // 2, give, 0, unroll=4)
    pairs[0].wait_recv()
    pair_sum(0)
    each_w([0], start)

    add_cross(chunks - 1)
    for j in range(1, count_band):
        cut(others + j, cross[j - 1])
        cut(j, cross[j - 1].T)
    pairs[1].start()
    lax.fori_loop(local // 2, local, give, 0, unroll=4)
    pairs[1].wait_recv()
    for n in range(1, 1 + 2 * others):
        pair_sum(n)
    cross_sends = [v_copy(j, k) for j in range(1, count_band) for k in range(per_block // 2)]
    for copy in cross_sends:
        copy.start()
    each_w(range(1, count_band), start)

    block = lax.div(e, per_block)
    margin_ref[...] = w2[lax.rem(block - b + count_band, count_band), pair - block * (per_block // 2)].astype(jnp.float32)
    for d in range(1, half):
        source = lax.rem(pair + d, half)
        pltpu.make_async_remote_copy(
            src_ref=w2.at[0, 0],
            dst_ref=rw.at[source],
            send_sem=w_send.at[0, 0],
            recv_sem=w_recv.at[source],
            device_id=(2 * source + parity, b),
            device_id_type=MESH,
        ).wait_recv()
        margin_ref[...] += rw[source].astype(jnp.float32)

    @pl.when(block != b)
    def _():
        for k in range(half):
            pltpu.make_async_remote_copy(
                src_ref=w2.at[0, 0],
                dst_ref=rv.at[k],
                send_sem=v_send.at[0, 0],
                recv_sem=v_recv.at[k],
                device_id=(2 * k + parity, block),
                device_id_type=MESH,
            ).wait_recv()
            margin_ref[...] += rv[k].astype(jnp.float32)

    margin_ref[...] = margin_ref[...] / jnp.float32(local * count_elem * bmax)

    for copy in pairs + cross_sends:
        copy.wait_send()
    each_w(range(count_band), sent)

    fast_copy(0, y1).wait_send()
    fast_copy(1, y2).wait_send()

    def drain(c, _):
        slow_copy(0, c, y1).wait_send()
        slow_copy(1, c, y2).wait_send()
        for j in range(1, count_band):
            x_copy(j, c).wait_send()
        return 0

    lax.fori_loop(0, chunks, drain, 0)


def on_device(count_elem, count_band, y_current, y_previous, h_blocks, basis_sizes, neighbours):
    local, bmax, bands = y_current.shape
    rows = bands * count_band // count_elem
    per_block = bands // rows
    half = count_elem // 2
    smem = pltpu.SMEM
    chunks = local // 2 // GROUP
    fixed = pl.BlockSpec(memory_space=pltpu.HBM)
    bf16, f32 = jnp.bfloat16, jnp.float32
    dma = pltpu.SemaphoreType.DMA
    whole = (local, bmax, bands)
    others = count_band - 1
    slot = (rows, bands)
    return tuple(pl.pallas_call(
        functools.partial(kernel, count_elem, count_band),
        out_shape=(
            jax.ShapeDtypeStruct(whole, bf16),
            jax.ShapeDtypeStruct((rows, bands), f32),
        ),
        in_specs=[fixed] * 5,
        out_specs=[pl.BlockSpec(memory_space=pltpu.VMEM)] * 2,
        scratch_shapes=[
            pltpu.VMEM((4, local), jnp.int32),
            pltpu.VMEM((8, 128), jnp.int32),
            smem((4, local), jnp.int32),
            smem((local,), jnp.int32),
            smem((8, 128), jnp.int32),
            pltpu.VMEM(whole, bf16),
            pltpu.VMEM(whole, bf16),
            pltpu.VMEM(h_blocks.shape, bf16),
            pltpu.VMEM(whole, bf16),
            pltpu.VMEM(whole, bf16),
            pltpu.VMEM(whole, bf16),
            pltpu.VMEM((2, 2, local // 2, bmax, bands), bf16),
            pltpu.VMEM((others, local // 2, bmax, bands), bf16),
            pltpu.VMEM((bands, bands), f32),
            pltpu.VMEM((others, bands, bands), f32),
            pltpu.VMEM((2, 1 + 2 * others, per_block // 2) + slot, bf16),
            pltpu.VMEM((1 + 2 * others, per_block // 2) + slot, bf16),
            pltpu.VMEM((1 + 2 * others, per_block // 2) + slot, bf16),
            pltpu.VMEM((half,) + slot, bf16),
            pltpu.VMEM((half,) + slot, bf16),
            dma((7,)),
            dma((2, chunks + 1)),
            dma((2, chunks + 1)),
            dma((others, chunks)),
            dma((others, chunks)),
            dma((2,)),
            dma((2,)),
            dma((count_band, per_block // 2)),
            dma((half,)),
            dma((others, per_block // 2)),
            dma((half,)),
            pltpu.SemaphoreType.REGULAR((count_elem.bit_length() + 1,)),
        ],
        compiler_params=pltpu.CompilerParams(
            collective_id=0, has_side_effects=True, vmem_limit_bytes=48 * 1024 * 1024
        ),
    )(*(
        pltpu.with_memory_space_constraint(array, pltpu.HBM)
        for array in (neighbours.T, basis_sizes, y_current, y_previous, h_blocks)
    )))


def solution(mesh):
    in_specs = (
        P("elem", None, "band"),
        P("elem", None, "band"),
        P("elem", None, None),
        P("elem"),
        P("elem", None),
    )
    out_specs = (P("elem", None, "band"), P("elem", "band"))
    body = functools.partial(on_device, mesh.shape["elem"], mesh.shape["band"])
    return jax.shard_map(body, mesh=mesh, in_specs=in_specs, out_specs=out_specs, check_vma=False)
```

```python
import functools

import jax
import jax.numpy as jnp
from jax import lax
from jax.experimental import pallas as pl
from jax.experimental.pallas import tpu as pltpu
from jax.sharding import PartitionSpec as P

GROUP = 4
center_value = 0.3
spectral_half = 1.7
MESH = pl.DeviceIdType.MESH
ROWS = (((0,), (0,)), ((), ()))


def kernel(
    count_elem, count_band,
    neigh_hbm, size_hbm, cur_hbm, prev_hbm, h_hbm,
    out_ref, margin_ref,
    neigh_vec, table_vec, neigh_ref, size_ref, table,
    cur, prev, h, y1, y2, f, halo, other, gram, cross,
    w, w1, w2, rw, rv,
    load_sem, halo_send, halo_recv, x_send, x_recv,
    pair_send, pair_recv, w_send, w_recv, v_send, v_recv, far,
):
    e = lax.axis_index("elem")
    b = lax.axis_index("band")
    local, bmax, bands = y1.shape
    edge = local // 2
    q = GROUP
    chunks = edge // q
    half = count_elem // 2
    rows = margin_ref.shape[0]
    per_block = bands // rows
    parity = lax.rem(e, 2)
    pair = lax.div(e, 2)
    fast, slow = 1 - parity, parity
    partner = e + 1 - 2 * parity
    neighbour = lax.rem(e + count_elem - 1 + 2 * parity, count_elem)

    sources = (neigh_hbm, neigh_hbm, size_hbm, cur_hbm, prev_hbm, h_hbm)
    targets = (neigh_vec, neigh_ref, size_ref, cur, prev, h)
    loads = [
        pltpu.make_async_copy(source, target, load_sem.at[k])
        for k, (source, target) in enumerate(zip(sources, targets))
    ]
    for load in loads[:4]:
        load.start()

    barrier = pltpu.get_barrier_semaphore()
    for target in (neighbour, partner):
        pl.semaphore_signal(barrier, inc=1, device_id=(target, b), device_id_type=MESH)
    for j in range(1, count_band):
        pl.semaphore_signal(
            barrier, inc=1, device_id=(e, lax.rem(b + j, count_band)), device_id_type=MESH
        )

    reach = [1]
    while 2 * reach[-1] < half:
        reach.append(2 * reach[-1])

    def advance(step):
        if 0 < step <= len(reach):
            pl.semaphore_wait(far.at[step - 1], 2)
        elif step == len(reach) + 1:
            pl.semaphore_wait(far.at[step - 1], count_band - 1)
        if step < len(reach):
            for distance in (reach[step], count_elem - reach[step]):
                target = (lax.rem(e + distance, count_elem), b)
                pl.semaphore_signal(far.at[step], inc=1, device_id=target, device_id_type=MESH)
        elif step == len(reach):
            for j in range(1, count_band):
                target = (e, lax.rem(b + j, count_band))
                pl.semaphore_signal(far.at[step], inc=1, device_id=target, device_id_type=MESH)

    loads[0].wait()
    above = neigh_vec[0:1, :]
    lane = lax.broadcasted_iota(jnp.int32, (1, local), 1)
    key = jnp.where(lax.div(above, local) != e, lax.rem(above, local), local + lane)
    key = key * local + lane
    key_row = jnp.broadcast_to(key, (local, local))
    down = lax.broadcasted_iota(jnp.int32, (local, local), 0)
    across = lax.broadcasted_iota(jnp.int32, (local, local), 1)
    key_col = jnp.sum(jnp.where(down == across, key_row, 0), axis=1, keepdims=True)
    pos_row = jnp.sum(jnp.where(key_col < key_row, 1, 0), axis=0, keepdims=True)
    pos_col = jnp.sum(jnp.where(key_row < key_col, 1, 0), axis=1, keepdims=True)
    perm_row = jnp.sum(jnp.where(pos_col == across, down, 0), axis=0, keepdims=True)
    table_vec[0:1, 0:local] = pos_row
    table_vec[1:2, 0:local] = perm_row
    order = pltpu.make_async_copy(table_vec, table, load_sem.at[len(loads)])
    order.start()

    row_index = lax.broadcasted_iota(jnp.int32, (bmax, bands), 0)

    for load in loads[1:4]:
        load.wait()
    for load in loads[4:]:
        load.start()
    order.wait()

    def place(start):
        def one(k, _):
            p = start + k
            i = table[1, p]
            y1[p] = jnp.where(row_index < size_ref[i], cur[i].astype(jnp.float32), 0.0).astype(jnp.bfloat16)
            return 0

        lax.fori_loop(0, edge, one, 0, unroll=4)

    def slow_copy(degree, c, source):
        return pltpu.make_async_remote_copy(
            src_ref=source.at[pl.ds(slow * edge + c * q, q)],
            dst_ref=halo.at[degree, 0, pl.ds(c * q, q)],
            send_sem=halo_send.at[degree, c],
            recv_sem=halo_recv.at[degree, c],
            device_id=(neighbour, b),
            device_id_type=MESH,
        )

    def fast_copy(degree, source):
        return pltpu.make_async_remote_copy(
            src_ref=source.at[pl.ds(fast * edge, edge)],
            dst_ref=halo.at[degree, 1],
            send_sem=halo_send.at[degree, chunks],
            recv_sem=halo_recv.at[degree, chunks],
            device_id=(partner, b),
            device_id_type=MESH,
        )

    place(slow * edge)
    pl.semaphore_wait(barrier, 1 + count_band)
    for c in range(chunks):
        slow_copy(0, c, y1).start()
    place(fast * edge)
    fast_copy(0, y1).start()
    advance(0)

    loads[4].wait()
    loads[5].wait()

    def element(degree, side, s, now, older, store):
        p = side * edge + s
        i = table[1, p]
        inner = now[table[0, lax.rem(neigh_ref[1 - side, i], local)]]
        left = now[table[0, lax.rem(neigh_ref[2, i], local)]]
        right = now[table[0, lax.rem(neigh_ref[3, i], local)]]
        outer = halo[degree, jnp.where(side == fast, 1, 0), s]
        mine = now[p]
        upper = jnp.where(side == 0, outer, inner)
        lower = jnp.where(side == 0, inner, outer)
        stacked = jnp.concatenate([mine, upper, lower, left, right], axis=0)
        applied = jnp.dot(h[i], stacked, preferred_element_type=jnp.float32)
        following = (2.0 / spectral_half) * (
            applied - center_value * mine.astype(jnp.float32)
        ) - older(p, i).astype(jnp.float32)
        store[p] = jnp.where(row_index < size_ref[i], following, 0.0).astype(jnp.bfloat16)

    def older_first(p, i):
        return prev[i]

    def older_second(p, i):
        return y1[p]

    def first_fast(g, _):
        for k in range(4):
            element(0, fast, g * 4 + k, y1, older_first, y2)
        return 0

    fast_copy(0, y1).wait_recv()
    lax.fori_loop(0, edge // 4, first_fast, 0)
    fast_copy(1, y2).start()
    advance(1)

    def first_slow(c, _):
        slow_copy(0, c, y1).wait_recv()
        for k in range(q):
            element(0, slow, c * q + k, y1, older_first, y2)
        slow_copy(1, c, y2).start()
        return 0

    lax.fori_loop(0, chunks, first_slow, 0)
    advance(2)

    gram[...] = jnp.zeros_like(gram)
    cross[...] = jnp.zeros_like(cross)

    def sent_side(j):
        return jnp.where(lax.rem(b + j, count_band) < b, 0, 1)

    def x_copy(j, c):
        return pltpu.make_async_remote_copy(
            src_ref=f.at[pl.ds(sent_side(j) * edge + c * q, q)],
            dst_ref=other.at[count_band - j - 1, pl.ds(c * q, q)],
            send_sem=x_send.at[j - 1, c],
            recv_sem=x_recv.at[count_band - j - 1, c],
            device_id=(e, lax.rem(b + j, count_band)),
            device_id_type=MESH,
        )

    def x_start(side, c):
        for j in range(1, count_band):
            @pl.when(sent_side(j) == side)
            def _():
                x_copy(j, c).start()

    def x_arrived(j, c):
        pltpu.make_async_remote_copy(
            src_ref=f.at[pl.ds(0, q)],
            dst_ref=other.at[j - 1, pl.ds(c * q, q)],
            send_sem=x_send.at[j - 1, c],
            recv_sem=x_recv.at[j - 1, c],
            device_id=(e, lax.rem(b + j, count_band)),
            device_id_type=MESH,
        ).wait_recv()

    def add_gram(first, count):
        block = f[pl.ds(first, count)].reshape(count * bmax, bands)
        gram[...] += lax.dot_general(block, block, ROWS, preferred_element_type=jnp.float32)

    def add_cross(c):
        for j in range(1, count_band):
            x_arrived(j, c)
            start = (1 - sent_side(j)) * edge
            mine = f[pl.ds(start + c * q, q)].reshape(q * bmax, bands)
            theirs = other[j - 1, pl.ds(c * q, q)].reshape(q * bmax, bands)
            cross[j - 1] += lax.dot_general(mine, theirs, ROWS, preferred_element_type=jnp.float32)

    fast_copy(1, y2).wait_recv()

    def second_fast(g, _):
        for k in range(4):
            element(1, fast, g * 4 + k, y2, older_second, f)
        for k in range(4 // q):
            x_start(fast, g * (4 // q) + k)
        return 0

    lax.fori_loop(0, edge // 4, second_fast, 0)
    advance(3)

    def gram_fast(g, _):
        add_gram(fast * edge + g * 4, 4)
        return 0

    lax.fori_loop(0, edge // 4, gram_fast, 0)

    def second_slow(c, _):
        slow_copy(1, c, y2).wait_recv()
        for k in range(q):
            element(1, slow, c * q + k, y2, older_second, f)
        x_start(slow, c)
        add_gram(slow * edge + c * q, q)

        @pl.when(c > 0)
        def _():
            add_cross(c - 1)

        return 0

    lax.fori_loop(0, chunks, second_slow, 0)

    def cut(target, matrix):
        for k in range(per_block):
            w[k % 2, target, k // 2] = matrix[k * rows:(k + 1) * rows].astype(jnp.bfloat16)

    def pair_copy(n, first, count):
        return pltpu.make_async_remote_copy(
            src_ref=w.at[1 - parity, pl.ds(first, count)],
            dst_ref=w1.at[pl.ds(first, count)],
            send_sem=pair_send.at[n],
            recv_sem=pair_recv.at[n],
            device_id=(partner, b),
            device_id_type=MESH,
        )

    def pair_sum(n):
        w2[n] = (w[parity, n].astype(jnp.float32) + w1[n].astype(jnp.float32)).astype(jnp.bfloat16)

    others = count_band - 1

    def far_first(k):
        return jnp.where(e < half, per_block // 2 - 1 - k, k)

    def w_copy(j, k):
        to = lax.rem(b + j, count_band) * (per_block // 2) + k
        return to, pltpu.make_async_remote_copy(
            src_ref=w2.at[j, k],
            dst_ref=rw.at[pair],
            send_sem=w_send.at[j, k],
            recv_sem=w_recv.at[pair],
            device_id=(2 * to + parity, b),
            device_id_type=MESH,
        )

    def v_copy(j, k):
        return pltpu.make_async_remote_copy(
            src_ref=w2.at[others + j, k],
            dst_ref=rv.at[pair],
            send_sem=v_send.at[j - 1, k],
            recv_sem=v_recv.at[pair],
            device_id=(b * per_block + 2 * k + parity, lax.rem(b + j, count_band)),
            device_id_type=MESH,
        )

    def each_w(blocks, act):
        for j in blocks:
            for k in range(per_block // 2):
                to, copy = w_copy(j, far_first(k))

                @pl.when(to != pair)
                def _():
                    act(copy)

    def start(copy):
        copy.start()

    def sent(copy):
        copy.wait_send()

    cut(0, gram[...])
    pairs = [pair_copy(0, 0, 1), pair_copy(1, 1 + others, others), pair_copy(2, 1, others)]
    pairs[0].start()

    for step in range(4, len(reach) + 2):
        advance(step)

    def give(i, _):
        out_ref[i] = f[table[0, i]]
        return 0

    lax.fori_loop(0, local, give, 0, unroll=4)
    pairs[0].wait_recv()
    pair_sum(0)
    each_w([0], start)

    add_cross(chunks - 1)
    for j in range(1, count_band):
        cut(others + j, cross[j - 1])
    pairs[1].start()
    for j in range(1, count_band):
        cut(j, cross[j - 1].T)
    pairs[2].start()
    pairs[1].wait_recv()
    for j in range(1, count_band):
        pair_sum(others + j)
    cross_sends = [v_copy(j, far_first(k)) for j in range(1, count_band) for k in range(per_block // 2)]
    for copy in cross_sends:
        copy.start()
    pairs[2].wait_recv()
    for j in range(1, count_band):
        pair_sum(j)
    each_w(range(1, count_band), start)

    block = lax.div(e, per_block)
    margin_ref[...] = w2[lax.rem(block - b + count_band, count_band), pair - block * (per_block // 2)].astype(jnp.float32)
    for d in range(1, half):
        source = lax.rem(pair + d, half)
        pltpu.make_async_remote_copy(
            src_ref=w2.at[0, 0],
            dst_ref=rw.at[source],
            send_sem=w_send.at[0, 0],
            recv_sem=w_recv.at[source],
            device_id=(2 * source + parity, b),
            device_id_type=MESH,
        ).wait_recv()
        margin_ref[...] += rw[source].astype(jnp.float32)

    @pl.when(block != b)
    def _():
        for k in range(half):
            pltpu.make_async_remote_copy(
                src_ref=w2.at[0, 0],
                dst_ref=rv.at[k],
                send_sem=v_send.at[0, 0],
                recv_sem=v_recv.at[k],
                device_id=(2 * k + parity, block),
                device_id_type=MESH,
            ).wait_recv()
            margin_ref[...] += rv[k].astype(jnp.float32)

    margin_ref[...] = margin_ref[...] / jnp.float32(local * count_elem * bmax)

    for copy in pairs + cross_sends:
        copy.wait_send()
    each_w(range(count_band), sent)

    fast_copy(0, y1).wait_send()
    fast_copy(1, y2).wait_send()

    def drain(c, _):
        slow_copy(0, c, y1).wait_send()
        slow_copy(1, c, y2).wait_send()
        for j in range(1, count_band):
            x_copy(j, c).wait_send()
        return 0

    lax.fori_loop(0, chunks, drain, 0)


def write_out(filtered, margin, filtered_out, margin_out, sem):
    copies = [
        pltpu.make_async_copy(filtered, filtered_out, sem.at[0]),
        pltpu.make_async_copy(margin, margin_out, sem.at[1]),
    ]
    for copy in copies:
        copy.start()
    for copy in copies:
        copy.wait()


def on_device(count_elem, count_band, y_current, y_previous, h_blocks, basis_sizes, neighbours):
    local, bmax, bands = y_current.shape
    rows = bands * count_band // count_elem
    per_block = bands // rows
    half = count_elem // 2
    smem = pltpu.SMEM
    chunks = local // 2 // GROUP
    fixed = pl.BlockSpec(memory_space=pltpu.HBM)
    bf16, f32 = jnp.bfloat16, jnp.float32
    dma = pltpu.SemaphoreType.DMA
    whole = (local, bmax, bands)
    others = count_band - 1
    slot = (rows, bands)
    results = pl.pallas_call(
        functools.partial(kernel, count_elem, count_band),
        out_shape=(
            jax.ShapeDtypeStruct(whole, bf16),
            jax.ShapeDtypeStruct((rows, bands), f32),
        ),
        in_specs=[fixed] * 5,
        out_specs=[pl.BlockSpec(memory_space=pltpu.VMEM)] * 2,
        scratch_shapes=[
            pltpu.VMEM((4, local), jnp.int32),
            pltpu.VMEM((8, 128), jnp.int32),
            smem((4, local), jnp.int32),
            smem((local,), jnp.int32),
            smem((8, 128), jnp.int32),
            pltpu.VMEM(whole, bf16),
            pltpu.VMEM(whole, bf16),
            pltpu.VMEM(h_blocks.shape, bf16),
            pltpu.VMEM(whole, bf16),
            pltpu.VMEM(whole, bf16),
            pltpu.VMEM(whole, bf16),
            pltpu.VMEM((2, 2, local // 2, bmax, bands), bf16),
            pltpu.VMEM((others, local // 2, bmax, bands), bf16),
            pltpu.VMEM((bands, bands), f32),
            pltpu.VMEM((others, bands, bands), f32),
            pltpu.VMEM((2, 1 + 2 * others, per_block // 2) + slot, bf16),
            pltpu.VMEM((1 + 2 * others, per_block // 2) + slot, bf16),
            pltpu.VMEM((1 + 2 * others, per_block // 2) + slot, bf16),
            pltpu.VMEM((half,) + slot, bf16),
            pltpu.VMEM((half,) + slot, bf16),
            dma((7,)),
            dma((2, chunks + 1)),
            dma((2, chunks + 1)),
            dma((others, chunks)),
            dma((others, chunks)),
            dma((3,)),
            dma((3,)),
            dma((count_band, per_block // 2)),
            dma((half,)),
            dma((others, per_block // 2)),
            dma((half,)),
            pltpu.SemaphoreType.REGULAR((count_elem.bit_length() + 1,)),
        ],
        compiler_params=pltpu.CompilerParams(
            collective_id=0, has_side_effects=True, vmem_limit_bytes=48 * 1024 * 1024
        ),
    )(*(
        pltpu.with_memory_space_constraint(array, pltpu.HBM)
        for array in (neighbours.T, basis_sizes, y_current, y_previous, h_blocks)
    ))
    anywhere = pl.BlockSpec(memory_space=pl.ANY)
    return tuple(pl.pallas_call(
        write_out,
        out_shape=[jax.ShapeDtypeStruct(array.shape, array.dtype) for array in results],
        in_specs=[pl.BlockSpec(memory_space=pltpu.VMEM)] * 2,
        out_specs=[anywhere] * 2,
        scratch_shapes=[dma((2,))],
    )(*(pltpu.with_memory_space_constraint(array, pltpu.VMEM) for array in results)))


def solution(mesh):
    in_specs = (
        P("elem", None, "band"),
        P("elem", None, "band"),
        P("elem", None, None),
        P("elem"),
        P("elem", None),
    )
    out_specs = (P("elem", None, "band"), P("elem", "band"))
    body = functools.partial(on_device, mesh.shape["elem"], mesh.shape["band"])
    return jax.shard_map(body, mesh=mesh, in_specs=in_specs, out_specs=out_specs, check_vma=False)
```

```python
import functools

import jax
import jax.numpy as jnp
from jax import lax
from jax.experimental import pallas as pl
from jax.experimental.pallas import tpu as pltpu
from jax.sharding import PartitionSpec as P

GROUP = 8
center_value = 0.3
spectral_half = 1.7
MESH = pl.DeviceIdType.MESH
ROWS = (((0,), (0,)), ((), ()))


def kernel(
    count_elem, count_band,
    neigh_hbm, size_hbm, cur_hbm, prev_hbm, h_hbm,
    out_ref, margin_ref,
    neigh_vec, table_vec, neigh_ref, size_ref, table,
    cur, prev, h, y1, y2, f, halo, other, gram, cross,
    w, w1, w2, rw, rv,
    load_sem, halo_send, halo_recv, x_send, x_recv,
    pair_send, pair_recv, w_send, w_recv, v_send, v_recv, far,
):
    e = lax.axis_index("elem")
    b = lax.axis_index("band")
    local, bmax, bands = y1.shape
    edge = local // 2
    q = GROUP
    chunks = edge // q
    half = count_elem // 2
    rows = margin_ref.shape[0]
    per_block = bands // rows
    parity = lax.rem(e, 2)
    pair = lax.div(e, 2)
    fast, slow = 1 - parity, parity
    partner = e + 1 - 2 * parity
    neighbour = lax.rem(e + count_elem - 1 + 2 * parity, count_elem)

    sources = (neigh_hbm, neigh_hbm, size_hbm, cur_hbm, prev_hbm, h_hbm)
    targets = (neigh_vec, neigh_ref, size_ref, cur, prev, h)
    loads = [
        pltpu.make_async_copy(source, target, load_sem.at[k])
        for k, (source, target) in enumerate(zip(sources, targets))
    ]
    for load in loads[:4]:
        load.start()

    barrier = pltpu.get_barrier_semaphore()
    for target in (neighbour, partner):
        pl.semaphore_signal(barrier, inc=1, device_id=(target, b), device_id_type=MESH)
    for j in range(1, count_band):
        pl.semaphore_signal(
            barrier, inc=1, device_id=(e, lax.rem(b + j, count_band)), device_id_type=MESH
        )

    reach = [1]
    while 2 * reach[-1] < half:
        reach.append(2 * reach[-1])

    def advance(step):
        if 0 < step <= len(reach):
            pl.semaphore_wait(far.at[step - 1], 2)
        elif step == len(reach) + 1:
            pl.semaphore_wait(far.at[step - 1], count_band - 1)
        if step < len(reach):
            for distance in (reach[step], count_elem - reach[step]):
                target = (lax.rem(e + distance, count_elem), b)
                pl.semaphore_signal(far.at[step], inc=1, device_id=target, device_id_type=MESH)
        elif step == len(reach):
            for j in range(1, count_band):
                target = (e, lax.rem(b + j, count_band))
                pl.semaphore_signal(far.at[step], inc=1, device_id=target, device_id_type=MESH)

    loads[0].wait()
    above = neigh_vec[0:1, :]
    lane = lax.broadcasted_iota(jnp.int32, (1, local), 1)
    key = jnp.where(lax.div(above, local) != e, lax.rem(above, local), local + lane)
    key = key * local + lane
    key_row = jnp.broadcast_to(key, (local, local))
    down = lax.broadcasted_iota(jnp.int32, (local, local), 0)
    across = lax.broadcasted_iota(jnp.int32, (local, local), 1)
    key_col = jnp.sum(jnp.where(down == across, key_row, 0), axis=1, keepdims=True)
    pos_row = jnp.sum(jnp.where(key_col < key_row, 1, 0), axis=0, keepdims=True)
    pos_col = jnp.sum(jnp.where(key_row < key_col, 1, 0), axis=1, keepdims=True)
    perm_row = jnp.sum(jnp.where(pos_col == across, down, 0), axis=0, keepdims=True)
    table_vec[0:1, 0:local] = pos_row
    table_vec[1:2, 0:local] = perm_row
    order = pltpu.make_async_copy(table_vec, table, load_sem.at[len(loads)])
    order.start()

    row_index = lax.broadcasted_iota(jnp.int32, (bmax, bands), 0)

    for load in loads[1:4]:
        load.wait()
    for load in loads[4:]:
        load.start()
    order.wait()

    def place(start):
        def one(k, _):
            p = start + k
            i = table[1, p]
            y1[p] = jnp.where(row_index < size_ref[i], cur[i].astype(jnp.float32), 0.0).astype(jnp.bfloat16)
            return 0

        lax.fori_loop(0, edge, one, 0, unroll=4)

    def slow_copy(degree, c, source):
        return pltpu.make_async_remote_copy(
            src_ref=source.at[pl.ds(slow * edge + c * q, q)],
            dst_ref=halo.at[degree, 0, pl.ds(c * q, q)],
            send_sem=halo_send.at[degree, c],
            recv_sem=halo_recv.at[degree, c],
            device_id=(neighbour, b),
            device_id_type=MESH,
        )

    def fast_copy(degree, source):
        return pltpu.make_async_remote_copy(
            src_ref=source.at[pl.ds(fast * edge, edge)],
            dst_ref=halo.at[degree, 1],
            send_sem=halo_send.at[degree, chunks],
            recv_sem=halo_recv.at[degree, chunks],
            device_id=(partner, b),
            device_id_type=MESH,
        )

    place(slow * edge)
    pl.semaphore_wait(barrier, 1 + count_band)
    for c in range(chunks):
        slow_copy(0, c, y1).start()
    place(fast * edge)
    fast_copy(0, y1).start()
    advance(0)

    loads[4].wait()
    loads[5].wait()

    def element(degree, side, s, now, older, store):
        p = side * edge + s
        i = table[1, p]
        inner = now[table[0, lax.rem(neigh_ref[1 - side, i], local)]]
        left = now[table[0, lax.rem(neigh_ref[2, i], local)]]
        right = now[table[0, lax.rem(neigh_ref[3, i], local)]]
        outer = halo[degree, jnp.where(side == fast, 1, 0), s]
        mine = now[p]
        upper = jnp.where(side == 0, outer, inner)
        lower = jnp.where(side == 0, inner, outer)
        stacked = jnp.concatenate([mine, upper, lower, left, right], axis=0)
        applied = jnp.dot(h[i], stacked, preferred_element_type=jnp.float32)
        following = (2.0 / spectral_half) * (
            applied - center_value * mine.astype(jnp.float32)
        ) - older(p, i).astype(jnp.float32)
        store[p] = jnp.where(row_index < size_ref[i], following, 0.0).astype(jnp.bfloat16)

    def older_first(p, i):
        return prev[i]

    def older_second(p, i):
        return y1[p]

    def first_fast(g, _):
        for k in range(4):
            element(0, fast, g * 4 + k, y1, older_first, y2)
        return 0

    fast_copy(0, y1).wait_recv()
    lax.fori_loop(0, edge // 4, first_fast, 0)
    fast_copy(1, y2).start()
    advance(1)

    def first_slow(c, _):
        slow_copy(0, c, y1).wait_recv()
        for k in range(q):
            element(0, slow, c * q + k, y1, older_first, y2)
        slow_copy(1, c, y2).start()
        return 0

    lax.fori_loop(0, chunks, first_slow, 0)
    advance(2)

    gram[...] = jnp.zeros_like(gram)
    cross[...] = jnp.zeros_like(cross)

    def sent_side(j):
        return jnp.where(lax.rem(b + j, count_band) < b, 0, 1)

    def x_copy(j, c):
        return pltpu.make_async_remote_copy(
            src_ref=f.at[pl.ds(sent_side(j) * edge + c * q, q)],
            dst_ref=other.at[count_band - j - 1, pl.ds(c * q, q)],
            send_sem=x_send.at[j - 1, c],
            recv_sem=x_recv.at[count_band - j - 1, c],
            device_id=(e, lax.rem(b + j, count_band)),
            device_id_type=MESH,
        )

    def x_start(side, c):
        for j in range(1, count_band):
            @pl.when(sent_side(j) == side)
            def _():
                x_copy(j, c).start()

    def x_arrived(j, c):
        pltpu.make_async_remote_copy(
            src_ref=f.at[pl.ds(0, q)],
            dst_ref=other.at[j - 1, pl.ds(c * q, q)],
            send_sem=x_send.at[j - 1, c],
            recv_sem=x_recv.at[j - 1, c],
            device_id=(e, lax.rem(b + j, count_band)),
            device_id_type=MESH,
        ).wait_recv()

    def add_gram(first, count):
        block = f[pl.ds(first, count)].reshape(count * bmax, bands)
        gram[...] += lax.dot_general(block, block, ROWS, preferred_element_type=jnp.float32)

    def add_cross(c):
        for j in range(1, count_band):
            x_arrived(j, c)
            start = (1 - sent_side(j)) * edge
            mine = f[pl.ds(start + c * q, q)].reshape(q * bmax, bands)
            theirs = other[j - 1, pl.ds(c * q, q)].reshape(q * bmax, bands)
            cross[j - 1] += lax.dot_general(mine, theirs, ROWS, preferred_element_type=jnp.float32)

    fast_copy(1, y2).wait_recv()

    def second_fast(g, _):
        for k in range(q):
            element(1, fast, g * q + k, y2, older_second, f)
        x_start(fast, g)
        return 0

    lax.fori_loop(0, chunks, second_fast, 0)
    advance(3)

    def gram_fast(g, _):
        add_gram(fast * edge + g * 4, 4)
        return 0

    lax.fori_loop(0, edge // 4, gram_fast, 0)

    def second_slow(c, _):
        slow_copy(1, c, y2).wait_recv()
        for k in range(q):
            element(1, slow, c * q + k, y2, older_second, f)
        x_start(slow, c)
        add_gram(slow * edge + c * q, q)

        @pl.when(c > 0)
        def _():
            add_cross(c - 1)

        return 0

    lax.fori_loop(0, chunks, second_slow, 0)

    def cut(target, matrix):
        for k in range(per_block):
            w[k % 2, target, k // 2] = matrix[k * rows:(k + 1) * rows].astype(jnp.bfloat16)

    def pair_copy(n, first, count):
        return pltpu.make_async_remote_copy(
            src_ref=w.at[1 - parity, pl.ds(first, count)],
            dst_ref=w1.at[pl.ds(first, count)],
            send_sem=pair_send.at[n],
            recv_sem=pair_recv.at[n],
            device_id=(partner, b),
            device_id_type=MESH,
        )

    def pair_sum(n):
        w2[n] = (w[parity, n].astype(jnp.float32) + w1[n].astype(jnp.float32)).astype(jnp.bfloat16)

    others = count_band - 1

    def far_first(k):
        return jnp.where(e < half, per_block // 2 - 1 - k, k)

    def w_copy(j, k):
        to = lax.rem(b + j, count_band) * (per_block // 2) + k
        return to, pltpu.make_async_remote_copy(
            src_ref=w2.at[j, k],
            dst_ref=rw.at[pair],
            send_sem=w_send.at[j, k],
            recv_sem=w_recv.at[pair],
            device_id=(2 * to + parity, b),
            device_id_type=MESH,
        )

    def v_copy(j, k):
        return pltpu.make_async_remote_copy(
            src_ref=w2.at[others + j, k],
            dst_ref=rv.at[pair],
            send_sem=v_send.at[j - 1, k],
            recv_sem=v_recv.at[pair],
            device_id=(b * per_block + 2 * k + parity, lax.rem(b + j, count_band)),
            device_id_type=MESH,
        )

    def each_w(blocks, act):
        for j in blocks:
            for k in range(per_block // 2):
                to, copy = w_copy(j, far_first(k))

                @pl.when(to != pair)
                def _():
                    act(copy)

    def start(copy):
        copy.start()

    def sent(copy):
        copy.wait_send()

    cut(0, gram[...])
    pairs = [pair_copy(0, 0, 1), pair_copy(1, 1 + others, others), pair_copy(2, 1, others)]
    pairs[0].start()

    for step in range(4, len(reach) + 2):
        advance(step)

    def give(i, _):
        out_ref[i] = f[table[0, i]]
        return 0

    lax.fori_loop(0, local, give, 0, unroll=4)
    pairs[0].wait_recv()
    pair_sum(0)
    each_w([0], start)

    add_cross(chunks - 1)
    for j in range(1, count_band):
        cut(others + j, cross[j - 1])
    pairs[1].start()
    for j in range(1, count_band):
        cut(j, cross[j - 1].T)
    pairs[2].start()
    pairs[1].wait_recv()
    for j in range(1, count_band):
        pair_sum(others + j)
    cross_sends = [v_copy(j, far_first(k)) for j in range(1, count_band) for k in range(per_block // 2)]
    for copy in cross_sends:
        copy.start()
    pairs[2].wait_recv()
    for j in range(1, count_band):
        pair_sum(j)
    each_w(range(1, count_band), start)

    block = lax.div(e, per_block)
    margin_ref[...] = w2[lax.rem(block - b + count_band, count_band), pair - block * (per_block // 2)].astype(jnp.float32)
    for d in range(1, half):
        source = lax.rem(pair + d, half)
        pltpu.make_async_remote_copy(
            src_ref=w2.at[0, 0],
            dst_ref=rw.at[source],
            send_sem=w_send.at[0, 0],
            recv_sem=w_recv.at[source],
            device_id=(2 * source + parity, b),
            device_id_type=MESH,
        ).wait_recv()
        margin_ref[...] += rw[source].astype(jnp.float32)

    @pl.when(block != b)
    def _():
        for k in range(half):
            pltpu.make_async_remote_copy(
                src_ref=w2.at[0, 0],
                dst_ref=rv.at[k],
                send_sem=v_send.at[0, 0],
                recv_sem=v_recv.at[k],
                device_id=(2 * k + parity, block),
                device_id_type=MESH,
            ).wait_recv()
            margin_ref[...] += rv[k].astype(jnp.float32)

    margin_ref[...] = margin_ref[...] / jnp.float32(local * count_elem * bmax)

    for copy in pairs + cross_sends:
        copy.wait_send()
    each_w(range(count_band), sent)

    fast_copy(0, y1).wait_send()
    fast_copy(1, y2).wait_send()

    def drain(c, _):
        slow_copy(0, c, y1).wait_send()
        slow_copy(1, c, y2).wait_send()
        for j in range(1, count_band):
            x_copy(j, c).wait_send()
        return 0

    lax.fori_loop(0, chunks, drain, 0)


def write_out(filtered, margin, filtered_out, margin_out, sem):
    copies = [
        pltpu.make_async_copy(filtered, filtered_out, sem.at[0]),
        pltpu.make_async_copy(margin, margin_out, sem.at[1]),
    ]
    for copy in copies:
        copy.start()
    for copy in copies:
        copy.wait()


def on_device(count_elem, count_band, y_current, y_previous, h_blocks, basis_sizes, neighbours):
    local, bmax, bands = y_current.shape
    rows = bands * count_band // count_elem
    per_block = bands // rows
    half = count_elem // 2
    smem = pltpu.SMEM
    chunks = local // 2 // GROUP
    fixed = pl.BlockSpec(memory_space=pltpu.HBM)
    bf16, f32 = jnp.bfloat16, jnp.float32
    dma = pltpu.SemaphoreType.DMA
    whole = (local, bmax, bands)
    others = count_band - 1
    slot = (rows, bands)
    results = pl.pallas_call(
        functools.partial(kernel, count_elem, count_band),
        out_shape=(
            jax.ShapeDtypeStruct(whole, bf16),
            jax.ShapeDtypeStruct((rows, bands), f32),
        ),
        in_specs=[fixed] * 5,
        out_specs=[pl.BlockSpec(memory_space=pltpu.VMEM)] * 2,
        scratch_shapes=[
            pltpu.VMEM((4, local), jnp.int32),
            pltpu.VMEM((8, 128), jnp.int32),
            smem((4, local), jnp.int32),
            smem((local,), jnp.int32),
            smem((8, 128), jnp.int32),
            pltpu.VMEM(whole, bf16),
            pltpu.VMEM(whole, bf16),
            pltpu.VMEM(h_blocks.shape, bf16),
            pltpu.VMEM(whole, bf16),
            pltpu.VMEM(whole, bf16),
            pltpu.VMEM(whole, bf16),
            pltpu.VMEM((2, 2, local // 2, bmax, bands), bf16),
            pltpu.VMEM((others, local // 2, bmax, bands), bf16),
            pltpu.VMEM((bands, bands), f32),
            pltpu.VMEM((others, bands, bands), f32),
            pltpu.VMEM((2, 1 + 2 * others, per_block // 2) + slot, bf16),
            pltpu.VMEM((1 + 2 * others, per_block // 2) + slot, bf16),
            pltpu.VMEM((1 + 2 * others, per_block // 2) + slot, bf16),
            pltpu.VMEM((half,) + slot, bf16),
            pltpu.VMEM((half,) + slot, bf16),
            dma((7,)),
            dma((2, chunks + 1)),
            dma((2, chunks + 1)),
            dma((others, chunks)),
            dma((others, chunks)),
            dma((3,)),
            dma((3,)),
            dma((count_band, per_block // 2)),
            dma((half,)),
            dma((others, per_block // 2)),
            dma((half,)),
            pltpu.SemaphoreType.REGULAR((count_elem.bit_length() + 1,)),
        ],
        compiler_params=pltpu.CompilerParams(
            collective_id=0, has_side_effects=True, vmem_limit_bytes=48 * 1024 * 1024
        ),
    )(*(
        pltpu.with_memory_space_constraint(array, pltpu.HBM)
        for array in (neighbours.T, basis_sizes, y_current, y_previous, h_blocks)
    ))
    anywhere = pl.BlockSpec(memory_space=pl.ANY)
    return tuple(pl.pallas_call(
        write_out,
        out_shape=[jax.ShapeDtypeStruct(array.shape, array.dtype) for array in results],
        in_specs=[pl.BlockSpec(memory_space=pltpu.VMEM)] * 2,
        out_specs=[anywhere] * 2,
        scratch_shapes=[dma((2,))],
    )(*(pltpu.with_memory_space_constraint(array, pltpu.VMEM) for array in results)))


def solution(mesh):
    in_specs = (
        P("elem", None, "band"),
        P("elem", None, "band"),
        P("elem", None, None),
        P("elem"),
        P("elem", None),
    )
    out_specs = (P("elem", None, "band"), P("elem", "band"))
    body = functools.partial(on_device, mesh.shape["elem"], mesh.shape["band"])
    return jax.shard_map(body, mesh=mesh, in_specs=in_specs, out_specs=out_specs, check_vma=False)
```
